256 devices in a mesh: param: 64 (over y, z, core), freq: 4 (over x).
Axes of the slice: x: 4, y: 4, z: 8, core: 2. Of those that a mesh axis runs over, the one named last changes fastest.
Arguments:
- kernel_hat: bfloat16 [2, 16, 600, 65536], P(None, 'freq', None, 'param'), may hold values from -0.25 to 0.25
- prior_gain: float32 [16, 65536], P('freq', 'param'), may hold values from 5.722046e-05 to 0.018310547, as said below
- noise_var: float32 [600], replicated, may hold values from 0.5 to 2
- observed: float32 [64, 16, 600], P('param', 'freq'), may hold values from -6 to 6
Outputs:
- solution: float32 [64, 16, 600], P('param', 'freq')
- residual: float32 [64, 16, 600], P('param', 'freq')
The draws below stay inside these ranges and needn't reach their ends.
Inputs may be any that keep to these rules, and one draw needn't show every extreme that they name: `prior_gain`: prior variances are positive.
All inputs are finite; a program needn't handle non-finite values.
Results may differ from the reference program's by a relative error of at most 0.0085.
Values may be sent and summed in bfloat16 or wider, within the bound.
A program may use at most 64 MiB of HBM per device.

```python
import math
import jax
import jax.numpy as jnp
from jax import lax

NS = 600
NT = 16
P_DEV = 1024
ITERS = 2
NP = 65536
R = 64


def draw_prior_gain(key, part):
    blocks = NP // P_DEV
    first_key, second_key = jax.random.split(jax.random.fold_in(key, 11))
    spread_base = jnp.exp(jax.random.uniform(first_key, (NT, NP), jnp.float32, jnp.log(0.2), jnp.log(2.0)))
    ranking = jax.random.permutation(second_key, blocks)
    weighty = (ranking < 2).astype(jnp.float32)
    factor = 1.0 + weighty * (0.5 * blocks - 1.0)
    overall = 0.5 * NS / (NT * NP)
    return (spread_base * jnp.repeat(factor, P_DEV)[None, :] * overall).astype(jnp.float32)


def shard_levels(rng, dims, shards, smallest, largest):
    factor_of, own = 1.0, jax.random.fold_in(rng, 6)
    for axis_at, shards_of in shards:
        draws = jnp.exp(jax.random.uniform(jax.random.fold_in(own, axis_at), (shards_of,), jnp.float32, smallest / len(shards), largest / len(shards)))
        factor_of = factor_of * jnp.repeat(draws, dims[axis_at] // shards_of).reshape([-1 if axis == axis_at else 1 for axis in range(len(dims))])
    return factor_of


def noise(own_key, shape, deviation, reach, cuts=(), kind=jnp.bfloat16):
    factor_of = shard_levels(own_key, shape, cuts, -0.22, 0.18) if cuts else 1.0
    result = jax.random.normal(own_key, shape, jnp.float32) * deviation * factor_of
    return jnp.minimum(jnp.maximum(result, -reach), reach).astype(kind)


def setup_inputs(seed: int = 0) -> dict:
    streams_of = jax.random.split(jax.random.key(seed), 5)
    return {
        "kernel_hat": noise(streams_of[0], (2, NT, NS, NP), NS ** -0.5, 0.25, ((1, 4), (3, 64))),
        "prior_gain": draw_prior_gain(jax.random.fold_in(streams_of[4], 71), 0),
        "noise_var": jnp.clip(jnp.exp(jax.random.uniform(streams_of[2], (NS,), jnp.float32, math.log(0.5), math.log(2.0))), 0.5, 2.0),
        "observed": noise(streams_of[3], (R, NT, NS), 1.0, 6.0, ((0, 64), (1, 4)), jnp.float32),
    }


HIGHEST = lax.Precision.HIGHEST


def phase_tables(freq_first, freq_count, time_first, time_count, period):
    freq_ids = freq_first + lax.iota(jnp.int32, freq_count)
    time_ids = time_first + lax.iota(jnp.int32, time_count)
    phase_int = (freq_ids[:, None] * time_ids[None, :]) % period
    phase = phase_int.astype(jnp.float32) * (2.0 * math.pi / period)
    return jnp.cos(phase), jnp.sin(phase)


def apply_hessian(fields, kernel_hat, prior_gain, noise_var):
    period = 2 * NT - 1
    cosines, sines = phase_tables(0, NT, 0, NT, period)
    spec_real = jnp.einsum("kt,rts->krs", cosines, fields, precision=HIGHEST).astype(jnp.bfloat16)
    spec_imag = (-jnp.einsum("kt,rts->krs", sines, fields, precision=HIGHEST)).astype(jnp.bfloat16)

    def one_slot(slot_id):
        real_part = kernel_hat[0, slot_id]
        imag_part = kernel_hat[1, slot_id]
        upper = spec_real[slot_id]
        lower = spec_imag[slot_id]
        coef_real = jnp.dot(upper, real_part, preferred_element_type=jnp.float32) + jnp.dot(lower, imag_part, preferred_element_type=jnp.float32)
        coef_imag = jnp.dot(lower, real_part, preferred_element_type=jnp.float32) - jnp.dot(upper, imag_part, preferred_element_type=jnp.float32)
        slot_gain = prior_gain[slot_id]
        coef_real = (coef_real * slot_gain[None, :]).astype(jnp.bfloat16)
        coef_imag = (coef_imag * slot_gain[None, :]).astype(jnp.bfloat16)
        image_real = jnp.dot(coef_real, real_part.T, preferred_element_type=jnp.float32) - jnp.dot(coef_imag, imag_part.T, preferred_element_type=jnp.float32)
        image_imag = jnp.dot(coef_imag, real_part.T, preferred_element_type=jnp.float32) + jnp.dot(coef_real, imag_part.T, preferred_element_type=jnp.float32)
        return image_real, image_imag

    image_real, image_imag = lax.map(one_slot, jnp.arange(NT, dtype=jnp.int32))
    inverse = jnp.einsum("krs,kt->rts", image_real, cosines, precision=HIGHEST) - jnp.einsum("krs,kt->rts", image_imag, sines, precision=HIGHEST)
    return noise_var[None, None, :] * fields + inverse


def reference(kernel_hat, prior_gain, noise_var, observed):
    solution = jnp.zeros_like(observed)
    residual = observed
    direction = observed
    norm_now = jnp.sum(residual * residual, axis=(1, 2))
    for sweep in range(ITERS):
        applied = apply_hessian(direction, kernel_hat, prior_gain, noise_var)
        step_len = norm_now / jnp.sum(direction * applied, axis=(1, 2))
        solution = solution + step_len[:, None, None] * direction
        residual = residual - step_len[:, None, None] * applied
        norm_next = jnp.sum(residual * residual, axis=(1, 2))
        direction = residual + (norm_next / norm_now)[:, None, None] * direction
        norm_now = norm_next
    return solution, residual
```

```python
import functools
import math

import jax
import jax.numpy as jnp
import numpy as np
from jax import lax
from jax.experimental import pallas as pl
from jax.experimental.pallas import tpu as pltpu
from jax.sharding import PartitionSpec as P

NT = 16
ITERS = 2
NX, NY, NZ = 4, 4, 8
SLOTS = NT // NX
NS = 600
LN = 640
TILES = LN // 128
PD = 1024
PERIOD = 2 * NT - 1
BF = jnp.bfloat16
F32 = jnp.float32
MESH = pl.DeviceIdType.MESH
NTDIMS = (((1,), (1,)), ((), ()))


def tables():
    k = np.arange(NT)[:, None]
    t = np.arange(NT)[None, :]
    phase = ((k * t) % PERIOD) * (2.0 * math.pi / PERIOD)
    cos, sin = np.cos(phase), np.sin(phase)
    forward = np.stack([cos.reshape(NX, SLOTS, NT), -sin.reshape(NX, SLOTS, NT)], axis=1)
    forward = forward.reshape(NX, 2 * SLOTS, NT).astype(np.float32)
    inverse = np.stack([cos, -sin], axis=1).reshape(2 * NT, NT).T.astype(np.float32)
    return forward, inverse


def kernel(
    k_hbm, gain, noise, obs, ftab, itab, sol_out, res_out,
    kbuf, obs_x, vd, vs, vr, zr, zst, sp, sbuf, cbuf, cneg, img, srecv, ysend, yrecv, ysum, zi, zri, xr,
    ksem, xo_s, xo_r, za_s, za_r, ya_s, ya_r, ss_s, ss_r, rs_s, rs_r, ry_s, ry_r, rz_s, rz_r, rx_s, rx_r,
):
    p = lax.axis_index("param")
    x = lax.axis_index("freq")
    core = lax.rem(p, 2)
    z = lax.rem(lax.div(p, 2), NZ)
    y = lax.div(p, 2 * NZ)

    def at(y_, z_, c_, x_):
        return ((y_ * NZ + z_) * 2 + c_, x_)

    def xpeer(j):
        return at(y, z, core, lax.rem(x + j, NX))

    def zpeer(j):
        return at(y, lax.rem(z + j, NZ), core, x)

    def ypeer(j):
        return at(lax.rem(y + j, NY), z, core, x)

    sibling = at(y, z, 1 - core, x)

    def remote(src, dst, ssem, rsem, dev):
        return pltpu.make_async_remote_copy(
            src_ref=src, dst_ref=dst, send_sem=ssem, recv_sem=rsem, device_id=dev, device_id_type=MESH
        )

    def kcopy(k, c):
        return pltpu.make_async_copy(k_hbm.at[c, k], kbuf.at[c, k], ksem.at[k, c])

    for k in range(SLOTS):
        for c in range(2):
            kcopy(k, c).start()

    barrier = pltpu.get_barrier_semaphore()
    partners = [xpeer(j) for j in range(1, NX)] + [zpeer(j) for j in range(1, NZ)]
    partners += [ypeer(j) for j in range(1, NY)] + [sibling]
    for dev in partners:
        pl.semaphore_signal(barrier, inc=1, device_id=dev, device_id_type=MESH)

    obs_x[x] = jnp.zeros((SLOTS, LN), F32)
    obs_x[x, :, :NS] = obs[0]
    pl.semaphore_wait(barrier, len(partners))

    def xo(j, who):
        return remote(obs_x.at[who], obs_x.at[who], xo_s.at[j - 1], xo_r.at[j - 1], xpeer(j))

    for j in range(1, NX):
        xo(j, x).start()
    for j in range(1, NX):
        xo(j, lax.rem(x + NX - j, NX)).wait_recv()
    for i in range(NX):
        vd[SLOTS * i : SLOTS * (i + 1), :] = obs_x[i]
    vr[...] = vd[...]
    vs[...] = jnp.zeros_like(vs)

    group = core * NY + y

    def za(it, j, who):
        return remote(zr.at[it, who], zr.at[it, who], za_s.at[it, j - 1], za_r.at[it, j - 1], zpeer(j))

    def ya(it, k, j, who):
        return remote(sp.at[it, k, who], sp.at[it, k, who], ya_s.at[it, k, j - 1], ya_r.at[it, k, j - 1], ypeer(j))

    def ss(it, k, j, who):
        return remote(sp.at[it, k, who], sp.at[it, k, who], ss_s.at[it, k, j], ss_r.at[it, k, j], sibling)

    def yfrom(j):
        return lax.rem(y + NY - j, NY)

    def rs(it, k):
        return remote(
            img.at[it, k, :, pl.ds((1 - core) * 32, 32), :], srecv.at[it, k], rs_s.at[it, k], rs_r.at[it, k], sibling
        )

    def ry(it, k, j):
        return remote(
            ysend.at[it, k, lax.rem(y + j, NY)], yrecv.at[it, k, j - 1], ry_s.at[it, k, j - 1], ry_r.at[it, k, j - 1], ypeer(j)
        )

    def rz(it, k, j):
        return remote(
            zi.at[it, k, lax.rem(z + j, NZ)], zri.at[it, k, j - 1], rz_s.at[it, k, j - 1], rz_r.at[it, k, j - 1], zpeer(j)
        )

    def rx(it, k, j, who):
        return remote(xr.at[it, who, k], xr.at[it, who, k], rx_s.at[it, k, j - 1], rx_r.at[it, k, j - 1], xpeer(j))

    def lay(who, item):
        for q in range(TILES):
            zst[q, pl.ds(pl.multiple_of(who * 8, 8), 8), :] = item[:, 128 * q : 128 * q + 128]

    def sweep(it, carry):
        table = ftab[x]
        d = vd[...]
        spec = table[:, 0:1] * d[0:1, :]
        for t in range(1, NT):
            spec = spec + table[:, t : t + 1] * d[t : t + 1, :]
        zr[it, z] = spec.astype(BF)
        for j in (4, 3, 5, 2, 6, 1, 7):
            za(it, j, z).start()
        lay(z, zr[it, z].astype(F32))
        for j in (1, 7, 2, 6, 3, 5, 4):
            who = lax.rem(z + NZ - j, NZ)
            za(it, j, who).wait_recv()
            lay(who, zr[it, who].astype(F32))
        for k in range(SLOTS):
            for q in range(TILES):
                up = zst[q, pl.ds(k, 8, stride=8), :]
                lo = zst[q, pl.ds(SLOTS + k, 8, stride=8), :]
                sp[it, k, group, :, 128 * q : 128 * q + 128] = jnp.concatenate([up, lo], axis=0).astype(BF)
            for j in (2, 1, 3):
                ya(it, k, j, group).start()
            ss(it, k, 0, group).start()

        def pass_on(k):
            for j in (1, 3, 2):
                who = core * NY + yfrom(j)
                ya(it, k, j, who).wait_recv()
                ss(it, k, j, who).start()

        def rs_one(k):
            rs(it, k).wait_recv()
            for yy in range(NY):
                own = img[it, k, :, pl.ds(pl.multiple_of(core * 32 + 8 * yy, 8), 8), :]
                both = own + srecv[it, k, :, 8 * yy : 8 * yy + 8, :]
                ysend[it, k, yy] = jnp.concatenate([both[0], both[1]], axis=0).astype(BF)
            for j in (2, 1, 3):
                ry(it, k, j).start()

        def slot(k, carry):
            @pl.when(k < SLOTS - 1)
            def _():
                pass_on(k + 1)

            for j in range(NY):
                ss(it, k, j, (1 - core) * NY + yfrom(j)).wait_recv()

            for c in range(2):
                for i in range(2):
                    for h in range(2):
                        g = c * NY + 2 * i + h
                        blk = sp[it, k, g]
                        row = c * 32 + 16 * i + 8 * h
                        blkf = blk.astype(F32)
                        zst2 = blkf
                        sbuf[row : row + 8, 0:LN] = zst2[0:8].astype(BF)
                        sbuf[row : row + 8, LN:] = zst2[8:16].astype(BF)
                        sbuf[64 + row : 64 + row + 8, 0:LN] = zst2[8:16].astype(BF)
                        sbuf[64 + row : 64 + row + 8, LN:] = (-zst2[0:8]).astype(BF)

            @pl.when(it == 0)
            def _():
                kcopy(k, 0).wait()
                kcopy(k, 1).wait()

            for n in range(PD // 256):
                cols = slice(256 * n, 256 * n + 256)
                coef = jnp.dot(sbuf[:, 0:NS], kbuf[0, k, :, cols], preferred_element_type=F32)
                coef = coef + jnp.dot(sbuf[:, LN : LN + NS], kbuf[1, k, :, cols], preferred_element_type=F32)
                coef = (coef * gain[pl.ds(k, 1), cols]).astype(BF)
                cbuf[:, cols] = coef
                cneg[0:64, cols] = -coef[64:128]
                cneg[64:128, cols] = coef[0:64]
            image = lax.dot_general(cbuf[...], kbuf[0, k], NTDIMS, preferred_element_type=F32)
            image = image + lax.dot_general(cneg[...], kbuf[1, k], NTDIMS, preferred_element_type=F32)
            img[it, k, 0, :, 0:NS] = image[0:64]
            img[it, k, 1, :, 0:NS] = image[64:128]
            img[it, k, 0, :, NS:LN] = jnp.zeros((64, LN - NS), F32)
            img[it, k, 1, :, NS:LN] = jnp.zeros((64, LN - NS), F32)
            rs(it, k).start()

            @pl.when(k > 0)
            def _():
                rs_one(k - 1)

            return carry

        pass_on(0)
        lax.fori_loop(0, SLOTS, slot, 0)
        rs_one(SLOTS - 1)

        def rs_two(k, carry):
            own = img[it, k, :, pl.ds(pl.multiple_of(core * 32 + 8 * y, 8), 8), :]
            own = own + srecv[it, k, :, pl.ds(pl.multiple_of(8 * y, 8), 8), :]
            total = jnp.concatenate([own[0], own[1]], axis=0)
            for j in (1, 3, 2):
                ry(it, k, j).wait_recv()
                total = total + yrecv[it, k, j - 1].astype(F32)
            for q in range(TILES):
                ysum[q] = total[:, 128 * q : 128 * q + 128]
            for zz in range(NZ):
                for q in range(TILES):
                    zi[it, k, zz, :, 128 * q : 128 * q + 128] = ysum[q, pl.ds(zz, 2, stride=8), :]
            for j in (4, 3, 5, 2, 6, 1, 7):
                rz(it, k, j).start()
            return carry

        lax.fori_loop(0, SLOTS, rs_two, 0)

        def rs_three(k, carry):
            total = zi[it, k, z]
            for j in (1, 7, 2, 6, 3, 5, 4):
                rz(it, k, j).wait_recv()
                total = total + zri[it, k, j - 1]
            xr[it, x, k] = total
            for j in (2, 1, 3):
                rx(it, k, j, x).start()
            return carry

        lax.fori_loop(0, SLOTS, rs_three, 0)
        d = vd[...]
        r = vr[...]
        rr = jnp.sum(r * r, keepdims=True)
        applied = nzv * d
        for j in (0, 1, 3, 2):
            who = lax.rem(x + NX - j, NX)
            for k in range(SLOTS):
                if j:
                    rx(it, k, j, who).wait_recv()
        back = itab[...]
        for i in range(NX):
            for k in range(SLOTS):
                two = xr[it, i, k]
                for c in range(2):
                    col = (i * SLOTS + k) * 2 + c
                    applied = applied + back[:, col : col + 1] * two[c : c + 1, :]
        step = rr / jnp.sum(d * applied, keepdims=True)
        vs[...] = vs[...] + step * d
        r = r - step * applied
        vr[...] = r
        fresh = jnp.sum(r * r, keepdims=True)
        vd[...] = r + (fresh / rr) * d
        return carry

    nzv = jnp.concatenate([noise[...], jnp.zeros((1, LN - NS), F32)], axis=1)
    lax.fori_loop(0, ITERS, sweep, 0)

    for i in range(NX):

        @pl.when(x == i)
        def _():
            sol_out[0] = vs[SLOTS * i : SLOTS * (i + 1), :NS]
            res_out[0] = vr[SLOTS * i : SLOTS * (i + 1), :NS]

    for j in range(1, NX):
        xo(j, x).wait_send()

    def drain(it, carry):
        for j in range(1, NZ):
            za(it, j, z).wait_send()

        def per_slot(k, carry):
            for j in range(1, NY):
                ya(it, k, j, group).wait_send()
                ry(it, k, j).wait_send()
            for j in range(NY):
                ss(it, k, j, group).wait_send()
            rs(it, k).wait_send()
            for j in range(1, NZ):
                rz(it, k, j).wait_send()
            for j in range(1, NX):
                rx(it, k, j, x).wait_send()
            return carry

        return lax.fori_loop(0, SLOTS, per_slot, carry)

    lax.fori_loop(0, ITERS, drain, 0)


def local(kernel_hat, prior_gain, noise_var, observed):
    forward, inverse = tables()
    vmem = pl.BlockSpec(memory_space=pltpu.VMEM)
    dma = pltpu.SemaphoreType.DMA
    v = pltpu.VMEM
    shape = jax.ShapeDtypeStruct(observed.shape, F32)
    return pl.pallas_call(
        kernel,
        out_shape=(shape, shape),
        in_specs=[pl.BlockSpec(memory_space=pl.ANY)] + [vmem] * 5,
        out_specs=(vmem, vmem),
        scratch_shapes=[
            v((2, SLOTS, NS, PD), BF),
            v((NX, SLOTS, LN), F32),
            v((NT, LN), F32),
            v((NT, LN), F32),
            v((NT, LN), F32),
            v((ITERS, NZ, 8, LN), BF),
            v((TILES, 64, 128), F32),
            v((ITERS, SLOTS, 8, 16, LN), BF),
            v((128, 2 * LN), BF),
            v((128, PD), BF),
            v((128, PD), BF),
            v((ITERS, SLOTS, 2, 64, LN), F32),
            v((ITERS, SLOTS, 2, 32, LN), F32),
            v((ITERS, SLOTS, NY, 16, LN), BF),
            v((ITERS, SLOTS, NY - 1, 16, LN), BF),
            v((TILES, 16, 128), F32),
            v((ITERS, SLOTS, NZ, 2, LN), F32),
            v((ITERS, SLOTS, NZ - 1, 2, LN), F32),
            v((ITERS, NX, SLOTS, 2, LN), F32),
            dma((SLOTS, 2)),
            dma((NX - 1,)),
            dma((NX - 1,)),
            dma((ITERS, NZ - 1)),
            dma((ITERS, NZ - 1)),
            dma((ITERS, SLOTS, NY - 1)),
            dma((ITERS, SLOTS, NY - 1)),
            dma((ITERS, SLOTS, NY)),
            dma((ITERS, SLOTS, NY)),
            dma((ITERS, SLOTS)),
            dma((ITERS, SLOTS)),
            dma((ITERS, SLOTS, NY - 1)),
            dma((ITERS, SLOTS, NY - 1)),
            dma((ITERS, SLOTS, NZ - 1)),
            dma((ITERS, SLOTS, NZ - 1)),
            dma((ITERS, SLOTS, NX - 1)),
            dma((ITERS, SLOTS, NX - 1)),
        ],
        compiler_params=pltpu.CompilerParams(
            collective_id=0, has_side_effects=True, vmem_limit_bytes=56 * 1024 * 1024
        ),
        name="cg",
    )(kernel_hat, prior_gain, noise_var.reshape(1, NS), observed, jnp.asarray(forward), jnp.asarray(inverse))


def solution(mesh):
    return jax.shard_map(
        local,
        mesh=mesh,
        in_specs=(
            P(None, "freq", None, "param"),
            P("freq", "param"),
            P(),
            P("param", "freq", None),
        ),
        out_specs=(P("param", "freq", None), P("param", "freq", None)),
        check_vma=False,
    )
```
